768 devices in a mesh: slab: 12 (over z), sub: 64 (over y, x, core).
Axes of the slice: x: 4, y: 8, z: 12, core: 2. Of those that a mesh axis runs over, the one named last changes fastest.
Arguments:
- near_null: float32 [18, 393216], P(None, ('slab', 'sub')), may hold values from -48 to 48
- aggregates: int32 [393216], P(('slab', 'sub')), may hold values from 0 to 63
- diag_block: float32 [9, 393216], P(None, ('slab', 'sub')), may hold values from -1 to 12, as said below
- off_blocks: float32 [26, 9, 393216], P(None, None, ('slab', 'sub')), may hold values from -18 to 18
- columns: int32 [26, 393216], P(None, ('slab', 'sub')), may hold values from 0 to 767, as said below
- sends: int32 [4, 49152], P(None, ('slab', 'sub')), may hold values from 0 to 511
- start_vector: float32 [3, 393216], P(None, ('slab', 'sub')), may hold values from -18 to 18
Outputs:
- prolong_off: bfloat16 [26, 18, 393216], P(None, None, ('slab', 'sub'))
- prolong_self: bfloat16 [18, 393216], P(None, ('slab', 'sub'))
- rho: float32 [], replicated
The draws below stay inside these ranges and needn't reach their ends.
Inputs may be any that keep to these rules, and one draw needn't show every extreme that they name: `diag_block`: each block, read as 3x3 row-major, is symmetric with diagonal entries between 6 and 12 and off-diagonal entries between -1 and 1. `columns`: entries below 512 name a node of the same device; an entry c of 512 or more names ghost slot c - 512. Row e lists, for each device, the local rows it sends to its neighbour at sub + 1, sub - 1, slab + 1, slab - 1 for e = 0, 1, 2, 3. `aggregates`: aggregates lie within one device.
All inputs are finite; a program needn't handle non-finite values.
Results may differ from the reference program's by a relative error of at most 0.001.
Values sent between devices are 32-bit elements; how exact they have to be, the bound alone decides.
No kernel may reach another device: no remote copies, remote signals or barrier semaphores. Data moves between devices by JAX's collectives and lax.ppermute only.
A program may use at most 32 MiB of HBM per device.

```python
import jax
import jax.numpy as jnp
from jax import lax

NB = 512
K = 26
ITERS = 8
GH = 64
AGG = 64
NODES = 393216
N_SLAB = 12
N_SUB = 64


def draw_diag_block(key, part):
    first_key, second_key = jax.random.split(key)
    middle = jax.random.uniform(first_key, (3, NODES), jnp.float32, 6.0, 12.0)
    side = jax.random.uniform(second_key, (3, NODES), jnp.float32, -1.0, 1.0)
    return jnp.stack([middle[0], side[0], side[1], side[0], middle[1], side[2], side[1], side[2], middle[2]])


def draw_start_vector(key, part):
    owner = (jnp.arange(NODES, dtype=jnp.int32) // NB).astype(jnp.float32)
    last_device = float(max(NODES // NB - 1, 1))
    base = jnp.clip(jax.random.normal(key, (3, NODES), jnp.float32), -6.0, 6.0)
    scale = 3.0 ** (owner / last_device)
    return base * scale[None, :]


def draw_columns(key, part):
    local_key, remote_key, pick_key = jax.random.split(jax.random.fold_in(key, 17), 3)
    nearby = jax.random.randint(local_key, (K, NODES), 0, NB, jnp.int32)
    remote = jax.random.randint(remote_key, (K, NODES), NB, NB + 4 * GH, jnp.int32)
    chooser = jax.random.randint(pick_key, (K, NODES), 0, 100, jnp.int32)
    result = jnp.where(chooser < 15, remote, nearby).astype(jnp.int32)
    result = result.at[0, 0].set(0)
    result = result.at[1, 0].set(NB + 4 * GH - 1)
    return result


def with_ends(drawn, own_key, smallest, top_value):
    place = [jax.random.randint(jax.random.fold_in(own_key, axis), (), 0, length) for axis, length in enumerate(drawn.shape)]
    main_axis = drawn.shape.index(max(drawn.shape))
    next_to = place[:main_axis] + [(place[main_axis] + 1) % drawn.shape[main_axis]] + place[main_axis + 1:]
    return drawn.at[tuple(place)].set(smallest).at[tuple(next_to)].set(top_value)


def levels(own_key, shape, pieces, smallest, largest):
    factor_of, own = 1.0, jax.random.fold_in(own_key, 6)
    for dim, parts in pieces:
        steps = jnp.exp(jax.random.uniform(jax.random.fold_in(own, dim), (parts,), jnp.float32, smallest / len(pieces), largest / len(pieces)))
        factor_of = factor_of * jnp.repeat(steps, shape[dim] // parts).reshape([-1 if axis == dim else 1 for axis in range(len(shape))])
    return factor_of


def bell_draw(own_key, shape, width, most, cuts=(), held_as=jnp.bfloat16):
    drawn = width * jax.random.normal(own_key, shape, jnp.float32)
    if cuts:
        drawn = drawn * levels(own_key, shape, cuts, -0.22, 0.18)
    return jnp.clip(drawn, -most, most).astype(held_as)


def setup_inputs(seed: int = 0) -> dict:
    arg_keys = jax.random.split(jax.random.key(seed), 8)
    near_null = bell_draw(arg_keys[0], (18, NODES), 8.0, 48.0, ((1, 768),), jnp.float32)
    aggregates = with_ends(jax.random.randint(arg_keys[1], (NODES,), 0, AGG), jax.random.fold_in(arg_keys[1], 1), 0, AGG - 1).astype(jnp.int32)
    diag_block = draw_diag_block(jax.random.fold_in(arg_keys[7], 71), 0)
    off_blocks = bell_draw(arg_keys[3], (K, 9, NODES), 3.0, 18.0, ((2, 768),), jnp.float32)
    columns = draw_columns(jax.random.fold_in(arg_keys[7], 71), 0)
    sends = with_ends(jax.random.randint(arg_keys[5], (4, GH * N_SLAB * N_SUB), 0, NB), jax.random.fold_in(arg_keys[5], 1), 0, NB - 1).astype(jnp.int32)
    start_vector = draw_start_vector(jax.random.fold_in(arg_keys[7], 71), 0)
    return {"near_null": near_null, "aggregates": aggregates, "diag_block": diag_block, "off_blocks": off_blocks, "columns": columns, "sends": sends, "start_vector": start_vector}


OMEGA = 4.0 / 3.0
HIGHEST = lax.Precision.HIGHEST

def invert_blocks(diag_block):
    entries = [diag_block[position] for position in range(9)]
    cofactor = [entries[4] * entries[8] - entries[5] * entries[7], entries[5] * entries[6] - entries[3] * entries[8], entries[3] * entries[7] - entries[4] * entries[6], entries[2] * entries[7] - entries[1] * entries[8], entries[0] * entries[8] - entries[2] * entries[6], entries[1] * entries[6] - entries[0] * entries[7], entries[1] * entries[5] - entries[2] * entries[4], entries[2] * entries[3] - entries[0] * entries[5], entries[0] * entries[4] - entries[1] * entries[3]]
    determinant = entries[0] * cofactor[0] + entries[1] * cofactor[1] + entries[2] * cofactor[2]
    inverse = [cofactor[column * 3 + row_index] / determinant for row_index in range(3) for column in range(3)]
    return jnp.stack(inverse).reshape((3, 3) + diag_block.shape[1:])

def reference(near_null, aggregates, diag_block, off_blocks, columns, sends, start_vector):
    device_count = N_SLAB * N_SUB
    ghost_count = NB // 8
    group_count = NB // 8
    node_number = jnp.arange(NODES, dtype=jnp.int32)
    owner = (node_number // NB).astype(jnp.int32)
    segment = owner * group_count + aggregates
    counts = jax.ops.segment_sum(jnp.ones((NODES,), jnp.float32), segment, num_segments=device_count * group_count)
    tentative = near_null * lax.rsqrt(counts[segment])[None, :]
    inverse = invert_blocks(diag_block)
    device_number = jnp.arange(device_count, dtype=jnp.int32)
    slab_index = device_number // N_SUB
    sub_index = device_number % N_SUB
    neighbours = [(slab_index, sub_index - 1), (slab_index, sub_index + 1), (slab_index - 1, sub_index), (slab_index + 1, sub_index)]
    send_rows = sends.reshape(4, device_count, ghost_count)
    tables = []
    valids = []
    for direction in range(4):
        slab_pos, sub_pos = neighbours[direction]
        present = (slab_pos >= 0) & (slab_pos < N_SLAB) & (sub_pos >= 0) & (sub_pos < N_SUB)
        sender = (jnp.clip(slab_pos, 0, N_SLAB - 1) * N_SUB + jnp.clip(sub_pos, 0, N_SUB - 1)).astype(jnp.int32)
        tables.append(sender[:, None] * NB + send_rows[direction][sender])
        valids.append(jnp.broadcast_to(present[:, None], (device_count, ghost_count)))
    table = jnp.concatenate(tables, axis=1).reshape(-1).astype(jnp.int32)
    valid = jnp.concatenate(valids, axis=1).reshape(-1)
    inside = columns < NB
    remote_slot = jnp.clip(columns - NB, 0, 4 * ghost_count - 1)
    flat_slot = (owner[None, :] * (4 * ghost_count) + remote_slot).astype(jnp.int32)
    source = jnp.where(inside, owner[None, :] * NB + columns, table[flat_slot]).astype(jnp.int32)
    weight = jnp.where(inside, True, valid[flat_slot]).astype(jnp.float32)
    mats = off_blocks.reshape(off_blocks.shape[0], 3, 3, NODES)

    def operator(field):

        def add_slot(total, slot_data):
            block, anchor, scale = slot_data
            picked = field[:, anchor] * scale[None, :]
            return (total + jnp.einsum('rcn,cmn->rmn', block, picked.reshape(3, 1, NODES), precision=HIGHEST), None)
        total, unused = lax.scan(add_slot, jnp.zeros((3, 1, NODES), jnp.float32), (mats, source, weight))
        return field + jnp.einsum('rcn,cmn->rmn', inverse, total, precision=HIGHEST).reshape(3, NODES)
    earlier = start_vector
    current = start_vector
    for iteration in range(ITERS):
        earlier = current
        current = operator(current)
    rho = jnp.sqrt(jnp.sum(current * current) / (jnp.sum(earlier * earlier) + 1e-05))

    def slot_blocks(slot_data):
        block, anchor, scale = slot_data
        picked = (tentative[:, anchor] * scale[None, :]).reshape(3, 6, NODES)
        product = jnp.einsum('rcn,cmn->rmn', block, picked, precision=HIGHEST)
        scaled = jnp.einsum('rcn,cmn->rmn', inverse, product, precision=HIGHEST)
        return (-(OMEGA / rho) * scaled).reshape(18, NODES).astype(jnp.bfloat16)
    prolong_off = lax.map(slot_blocks, (mats, source, weight))
    prolong_self = ((1.0 - OMEGA / rho) * tentative).astype(jnp.bfloat16)
    return (prolong_off, prolong_self, rho)
```

```python
import functools

import jax
import jax.numpy as jnp
from jax import lax
from jax.experimental import pallas as pl
from jax.experimental.pallas import tpu as pltpu
from jax.sharding import Mesh
from jax.sharding import PartitionSpec as P

ITERS = 8
OMEGA = 4.0 / 3.0
SUB = ("sub_0", "sub_1", "sub_2")
SLAB_SUB = ("slab", "sub_0", "sub_1", "sub_2")
LANES = 128
F32 = jnp.float32
VM = pl.BlockSpec(memory_space=pltpu.VMEM)


def lanes(group):
    return slice(group * LANES, (group + 1) * LANES)


def pick(sources, low, high):
    result = jnp.take_along_axis(sources[0], low, axis=1, mode="promise_in_bounds")
    for group in range(1, len(sources)):
        found = jnp.take_along_axis(sources[group], low, axis=1, mode="promise_in_bounds")
        result = jnp.where(high == group, found, result)
    return result


def spread(row):
    return jnp.broadcast_to(row, (8, LANES))


def pack_rows(table_ref, tiles, send_ref, pay_refs):
    for pay_ref, first in zip(pay_refs, (0, 1)):
        index = spread(send_ref[first : first + 1, :])
        low, high = index & (LANES - 1), index >> 7
        for tile in range(tiles):
            rows = slice(tile * 8, tile * 8 + 8)
            sources = [table_ref[rows, lanes(group)] for group in range(4)]
            pay_ref[rows, :] = pick(sources, low, high)


def start_kernel(near_ref, aggregates_ref, start_ref, sends_ref, table_ref, w_ref, send_ref, a_ref, b_ref):
    nodes = near_ref.shape[1]
    groups = nodes // 8
    for e in range(4):
        send_ref[e // 2 : e // 2 + 1, (e % 2) * 64 : (e % 2) * 64 + 64] = sends_ref[e : e + 1, :]
    name = lax.broadcasted_iota(jnp.int32, (groups, nodes), 0)
    members = (name == aggregates_ref[...]).astype(F32)
    sizes = jnp.sum(members, axis=1, keepdims=True)
    scale = lax.rsqrt(jnp.sum(members * sizes, axis=0, keepdims=True))
    table_ref[...] = jnp.zeros(table_ref.shape, F32)
    w_ref[...] = jnp.zeros(w_ref.shape, F32)
    for row in range(3):
        table_ref[row * 8 : row * 8 + 6, :] = near_ref[row * 6 : row * 6 + 6, :] * scale
        table_ref[row * 8 + 6 : row * 8 + 7, :] = start_ref[row : row + 1, :]
    w_ref[0:3, :] = start_ref[...]
    pack_rows(table_ref, 3, send_ref, (a_ref, b_ref))


def blocks_kernel(diag_ref, off_ref, columns_ref, scaled_ref, index_ref):
    slots = off_ref.shape[1]
    index_ref[0:slots, :] = columns_ref[...]
    index_ref[slots:, :] = jnp.zeros((index_ref.shape[0] - slots, index_ref.shape[1]), jnp.int32)
    scaled_ref[:, slots:, :] = jnp.zeros(
        (9, scaled_ref.shape[1] - slots, scaled_ref.shape[2]), F32
    )
    entries = [diag_ref[position : position + 1, :] for position in range(9)]
    cofactor = [
        entries[4] * entries[8] - entries[5] * entries[7],
        entries[5] * entries[6] - entries[3] * entries[8],
        entries[3] * entries[7] - entries[4] * entries[6],
        entries[2] * entries[7] - entries[1] * entries[8],
        entries[0] * entries[8] - entries[2] * entries[6],
        entries[1] * entries[6] - entries[0] * entries[7],
        entries[1] * entries[5] - entries[2] * entries[4],
        entries[2] * entries[3] - entries[0] * entries[5],
        entries[0] * entries[4] - entries[1] * entries[3],
    ]
    determinant = entries[0] * cofactor[0] + entries[1] * cofactor[1] + entries[2] * cofactor[2]
    inverse = [
        [cofactor[column * 3 + row] / determinant for column in range(3)] for row in range(3)
    ]
    for column in range(3):
        block = [off_ref[inner * 3 + column] for inner in range(3)]
        for row in range(3):
            total = inverse[row][0] * block[0]
            total = total + inverse[row][1] * block[1]
            total = total + inverse[row][2] * block[2]
            scaled_ref[row * 3 + column, 0:slots, :] = total


def ghost_row(refs, side_ref, axis, row):
    even, odd = refs
    use_odd = side_ref[axis : axis + 1, :] != 0
    return jnp.where(use_odd, odd[row : row + 1, :], even[row : row + 1, :])


def step_kernel(first, last, count, *refs):
    scaled_ref, index_ref, w_ref, ae, ao, be, bo, side_ref, send_ref = refs[:9]
    outs = refs[9:]
    next_ref = outs[0]
    table = []
    for c in range(3):
        row = c * 8 + 6 if first else c
        table.append(
            [spread(w_ref[c : c + 1, lanes(group)]) for group in range(4)]
            + [
                spread(ghost_row((ae, ao), side_ref, 0, row)),
                spread(ghost_row((be, bo), side_ref, 1, row)),
            ]
        )
    next_ref[...] = jnp.zeros(next_ref.shape, F32)
    for block in range(4):
        total = [None] * 3
        for tile in range(4):
            slots = slice(tile * 8, tile * 8 + 8)
            index = index_ref[slots, lanes(block)]
            low, high = index & (LANES - 1), index >> 7
            for c in range(3):
                found = pick(table[c], low, high)
                for r in range(3):
                    term = scaled_ref[r * 3 + c, slots, lanes(block)] * found
                    total[r] = term if total[r] is None else total[r] + term
        for r in range(3):
            next_ref[r : r + 1, lanes(block)] = w_ref[r : r + 1, lanes(block)] + jnp.sum(
                total[r], axis=0, keepdims=True
            )
    if last:
        sums_ref = outs[1]
        latest = jnp.sum(next_ref[...] * next_ref[...], keepdims=True)
        earlier = jnp.sum(w_ref[...] * w_ref[...], keepdims=True)
        lane = lax.broadcasted_iota(jnp.int32, (1, LANES), 1)
        both = jnp.where(lane == 0, latest, jnp.where(lane == 1, earlier, 0.0))
        sums_ref[...] = jnp.broadcast_to(both, (count, LANES))
    else:
        pack_rows(next_ref, 1, send_ref, outs[1:3])


def blocks_out_kernel(scaled_ref, index_ref, table_ref, ae, ao, be, bo, side_ref, out_ref):
    slots = out_ref.shape[1]
    use_odd = [side_ref[axis : axis + 1, :] != 0 for axis in range(2)]
    for block in range(4):
        for first in range(0, slots, 8):
            count = min(8, slots - first)
            tile = slice(first, first + 8)
            index = index_ref[tile, lanes(block)]
            low, high = index & (LANES - 1), index >> 7
            for m in range(6):
                found = []
                for c in range(3):
                    row = slice(c * 8 + m, c * 8 + m + 1)
                    sources = [spread(table_ref[row, lanes(group)]) for group in range(4)]
                    sources.append(spread(jnp.where(use_odd[0], ao[row, :], ae[row, :])))
                    sources.append(spread(jnp.where(use_odd[1], bo[row, :], be[row, :])))
                    found.append(pick(sources, low, high))
                for r in range(3):
                    total = None
                    for c in range(3):
                        term = scaled_ref[r * 3 + c, tile, lanes(block)] * found[c]
                        total = term if total is None else total + term
                    out_ref[r * 6 + m, first : first + count, lanes(block)] = total[0:count, :]


def regroup_kernel(sums_ref, out_ref):
    total = jnp.sum(sums_ref[...], axis=0, keepdims=True)
    out_ref[...] = jnp.broadcast_to(total, out_ref.shape)


def finish_kernel(sums_ref, raw_ref, table_ref, off_ref, self_ref, rho_ref):
    total = jnp.sum(sums_ref[...], axis=0, keepdims=True)
    lane = lax.broadcasted_iota(jnp.int32, (1, LANES), 1)
    latest = jnp.sum(jnp.where(lane == 0, total, 0.0), keepdims=True)
    earlier = jnp.sum(jnp.where(lane == 1, total, 0.0), keepdims=True)
    rho = jnp.sqrt(latest / (earlier + 1e-05))
    rho_ref[...] = jnp.broadcast_to(rho, rho_ref.shape)
    factor = -(OMEGA / rho)
    for entry in range(raw_ref.shape[0]):
        off_ref[entry] = (factor * raw_ref[entry]).astype(jnp.bfloat16)
    keep = 1.0 - OMEGA / rho
    for row in range(3):
        self_ref[row * 6 : row * 6 + 6, :] = (keep * table_ref[row * 8 : row * 8 + 6, :]).astype(
            jnp.bfloat16
        )


def call(kernel, name, outs, *args):
    return pl.pallas_call(
        kernel,
        name=name,
        out_shape=[
            jax.ShapeDtypeStruct(*out) if len(out) == 2 else pltpu.VMEM(*out[:2]) for out in outs
        ],
        in_specs=[VM] * len(args),
        out_specs=[VM] * len(outs),
        compiler_params=pltpu.CompilerParams(vmem_limit_bytes=16 << 20),
    )(*args)


def kept(array):
    return pltpu.with_memory_space_constraint(array, pltpu.VMEM)


def swap(count, offset):
    pairs = []
    for i in range(offset, count - 1, 2):
        pairs += [(i, i + 1), (i + 1, i)]
    return pairs


def exchange(a, b):
    subs, slabs = lax.axis_size(SUB), lax.axis_size("slab")
    ao = lax.ppermute(a, SUB, swap(subs, 1))
    be = lax.ppermute(b, "slab", swap(slabs, 0))
    bo = lax.ppermute(b, "slab", swap(slabs, 1))
    ae = lax.ppermute(a, SUB, swap(subs, 0))
    return ae, ao, be, bo


def body(near_null, aggregates, diag_block, off_blocks, columns, sends, start_vector):
    nodes = near_null.shape[1]
    slots = off_blocks.shape[0]
    padded = (slots + 7) // 8 * 8
    subs, slabs = lax.axis_size(SUB), lax.axis_size("slab")
    lane = jnp.arange(LANES, dtype=jnp.int32)[None, :]
    position = jnp.stack([lax.axis_index(SUB), lax.axis_index("slab")])[:, None] % 2
    side = ((lane < 64) == (position == 0)).astype(jnp.int32)

    kept_f32 = lambda *shape: (shape, F32, "kept")
    kept_i32 = lambda *shape: (shape, jnp.int32, "kept")
    table, w, send, a, b = call(
        start_kernel,
        "start",
        [kept_f32(24, nodes), kept_f32(8, nodes), kept_i32(2, LANES)]
        + [kept_f32(24, LANES)] * 2,
        near_null,
        aggregates[None, :],
        start_vector,
        sends,
    )
    received = [kept(x) for x in exchange(a, b)]
    side = kept(side)
    scaled, index = call(
        blocks_kernel,
        "blocks",
        [kept_f32(9, padded, nodes), kept_i32(padded, nodes)],
        diag_block,
        jnp.transpose(off_blocks, (1, 0, 2)),
        columns,
    )
    first_received = received
    for iteration in range(ITERS):
        last = iteration == ITERS - 1
        outs = [kept_f32(8, nodes)]
        outs += [kept_f32(subs, LANES)] if last else [kept_f32(8, LANES)] * 2
        result = call(
            functools.partial(step_kernel, iteration == 0, last, subs),
            f"step_{iteration}",
            outs,
            kept(scaled),
            kept(index),
            kept(w),
            *received,
            side,
            kept(send),
        )
        w = result[0]
        if last:
            sums = result[1]
        else:
            received = [kept(x) for x in exchange(result[1], result[2])]
    (raw,) = call(
        blocks_out_kernel,
        "blocks_out",
        [kept_f32(18, slots, nodes)],
        kept(scaled),
        kept(index),
        kept(table),
        *first_received,
        side,
    )
    sums = lax.all_to_all(sums, SUB, 0, 0, tiled=True)
    (sums,) = call(regroup_kernel, "regroup", [kept_f32(slabs, LANES)], kept(sums))
    sums = lax.all_to_all(sums, "slab", 0, 0, tiled=True)
    prolong_off, prolong_self, rho = call(
        finish_kernel,
        "finish",
        [((18, slots, nodes), jnp.bfloat16), ((18, nodes), jnp.bfloat16), ((1, LANES), F32)],
        kept(sums),
        kept(raw),
        kept(table),
    )
    return (jnp.transpose(prolong_off, (1, 0, 2)), prolong_self, rho[0, 0])


def solution(mesh):
    torus = Mesh(
        mesh.devices.reshape(mesh.shape["slab"], 8, 4, 2), ("slab", "sub_0", "sub_1", "sub_2")
    )
    placed = (
        P(None, SLAB_SUB),
        P(SLAB_SUB),
        P(None, SLAB_SUB),
        P(None, None, SLAB_SUB),
        P(None, SLAB_SUB),
        P(None, SLAB_SUB),
        P(None, SLAB_SUB),
    )
    return jax.shard_map(
        body,
        mesh=torus,
        in_specs=placed,
        out_specs=(P(None, None, SLAB_SUB), P(None, SLAB_SUB), P()),
        check_vma=False,
    )
```

```python
import functools

import jax
import jax.numpy as jnp
from jax import lax
from jax.experimental import pallas as pl
from jax.experimental.pallas import tpu as pltpu
from jax.sharding import Mesh
from jax.sharding import PartitionSpec as P

ITERS = 8
OMEGA = 4.0 / 3.0
SUB = ("sub_0", "sub_1", "sub_2")
SLAB_SUB = ("slab", "sub_0", "sub_1", "sub_2")
LANES = 128
F32 = jnp.float32
MODE = "square"
RECEIVED = {"perm": 4, "core": 4, "square": 3}[MODE]
VM = pl.BlockSpec(memory_space=pltpu.VMEM)


def lanes(group):
    return slice(group * LANES, (group + 1) * LANES)


def pick(sources, low, high):
    result = jnp.take_along_axis(sources[0], low, axis=1, mode="promise_in_bounds")
    for group in range(1, len(sources)):
        found = jnp.take_along_axis(sources[group], low, axis=1, mode="promise_in_bounds")
        result = jnp.where(high == group, found, result)
    return result


def spread(row):
    return jnp.broadcast_to(row, (8, LANES))


def pack_rows(table_ref, tiles, send_ref, pay_refs, both_ref):
    for pay_ref, first in zip(pay_refs, (0, 1)):
        index = spread(send_ref[first : first + 1, :])
        low, high = index & (LANES - 1), index >> 7
        for tile in range(tiles):
            rows = slice(tile * 8, tile * 8 + 8)
            sources = [table_ref[rows, lanes(group)] for group in range(4)]
            pay_ref[rows, :] = pick(sources, low, high)
    both_ref[0 : tiles * 8, :] = pay_refs[0][...]
    both_ref[tiles * 8 :, :] = pay_refs[1][...]


def start_kernel(near_ref, aggregates_ref, start_ref, sends_ref, table_ref, w_ref, send_ref, a_ref, b_ref, both_ref):
    nodes = near_ref.shape[1]
    groups = nodes // 8
    for e in range(4):
        send_ref[e // 2 : e // 2 + 1, (e % 2) * 64 : (e % 2) * 64 + 64] = sends_ref[e : e + 1, :]
    name = lax.broadcasted_iota(jnp.int32, (groups, nodes), 0)
    members = (name == aggregates_ref[...]).astype(F32)
    sizes = jnp.sum(members, axis=1, keepdims=True)
    scale = lax.rsqrt(jnp.sum(members * sizes, axis=0, keepdims=True))
    table_ref[...] = jnp.zeros(table_ref.shape, F32)
    w_ref[...] = jnp.zeros(w_ref.shape, F32)
    for row in range(3):
        table_ref[row * 8 : row * 8 + 6, :] = near_ref[row * 6 : row * 6 + 6, :] * scale
        table_ref[row * 8 + 6 : row * 8 + 7, :] = start_ref[row : row + 1, :]
    w_ref[0:3, :] = start_ref[...]
    pack_rows(table_ref, 3, send_ref, (a_ref, b_ref), both_ref)


def blocks_kernel(diag_ref, off_ref, columns_ref, scaled_ref, index_ref):
    slots = off_ref.shape[1]
    index_ref[0:slots, :] = columns_ref[...]
    index_ref[slots:, :] = jnp.zeros((index_ref.shape[0] - slots, index_ref.shape[1]), jnp.int32)
    scaled_ref[:, slots:, :] = jnp.zeros(
        (9, scaled_ref.shape[1] - slots, scaled_ref.shape[2]), F32
    )
    entries = [diag_ref[position : position + 1, :] for position in range(9)]
    cofactor = [
        entries[4] * entries[8] - entries[5] * entries[7],
        entries[5] * entries[6] - entries[3] * entries[8],
        entries[3] * entries[7] - entries[4] * entries[6],
        entries[2] * entries[7] - entries[1] * entries[8],
        entries[0] * entries[8] - entries[2] * entries[6],
        entries[1] * entries[6] - entries[0] * entries[7],
        entries[1] * entries[5] - entries[2] * entries[4],
        entries[2] * entries[3] - entries[0] * entries[5],
        entries[0] * entries[4] - entries[1] * entries[3],
    ]
    determinant = entries[0] * cofactor[0] + entries[1] * cofactor[1] + entries[2] * cofactor[2]
    inverse = [
        [cofactor[column * 3 + row] / determinant for column in range(3)] for row in range(3)
    ]
    for column in range(3):
        block = [off_ref[inner * 3 + column] for inner in range(3)]
        for row in range(3):
            total = inverse[row][0] * block[0]
            total = total + inverse[row][1] * block[1]
            total = total + inverse[row][2] * block[2]
            scaled_ref[row * 3 + column, 0:slots, :] = total


def ghost_rows(refs, side_ref, row):
    if MODE == "perm":
        ae, ao, be, bo = refs
        even = ae[row, :], be[row, :]
        odd = ao[row, :], bo[row, :]
    elif MODE == "core":
        ao, be, bo, gathered = refs
        odd_sub = side_ref[2:3, :] != 0
        even = jnp.where(odd_sub, gathered[0, row, :], gathered[1, row, :]), be[row, :]
        odd = ao[row, :], bo[row, :]
    else:
        ao, bo, gathered = refs
        odd_sub = side_ref[2:3, :] != 0
        odd_slab = side_ref[3:4, :] != 0
        half = gathered.shape[1] // 2
        down = slice(row.start + half, row.stop + half)
        even_a = jnp.where(
            odd_slab,
            jnp.where(odd_sub, gathered[2, row, :], gathered[3, row, :]),
            jnp.where(odd_sub, gathered[0, row, :], gathered[1, row, :]),
        )
        even_b = jnp.where(
            odd_slab,
            jnp.where(odd_sub, gathered[1, down, :], gathered[0, down, :]),
            jnp.where(odd_sub, gathered[3, down, :], gathered[2, down, :]),
        )
        even = even_a, even_b
        odd = ao[row, :], bo[row, :]
    return [
        spread(jnp.where(side_ref[axis : axis + 1, :] != 0, odd[axis], even[axis]))
        for axis in range(2)
    ]


def step_kernel(first, last, count, *refs):
    scaled_ref, index_ref, w_ref, side_ref, send_ref = refs[:5]
    received = refs[5 : 5 + RECEIVED]
    outs = refs[5 + RECEIVED :]
    next_ref = outs[0]
    table = []
    for c in range(3):
        row = c * 8 + 6 if first else c
        table.append(
            [spread(w_ref[c : c + 1, lanes(group)]) for group in range(4)]
            + ghost_rows(received, side_ref, slice(row, row + 1))
        )
    next_ref[...] = jnp.zeros(next_ref.shape, F32)
    for block in range(4):
        total = [None] * 3
        for tile in range(4):
            slots = slice(tile * 8, tile * 8 + 8)
            index = index_ref[slots, lanes(block)]
            low, high = index & (LANES - 1), index >> 7
            for c in range(3):
                found = pick(table[c], low, high)
                for r in range(3):
                    term = scaled_ref[r * 3 + c, slots, lanes(block)] * found
                    total[r] = term if total[r] is None else total[r] + term
        for r in range(3):
            next_ref[r : r + 1, lanes(block)] = w_ref[r : r + 1, lanes(block)] + jnp.sum(
                total[r], axis=0, keepdims=True
            )
    if last:
        sums_ref = outs[1]
        latest = jnp.sum(next_ref[...] * next_ref[...], keepdims=True)
        earlier = jnp.sum(w_ref[...] * w_ref[...], keepdims=True)
        lane = lax.broadcasted_iota(jnp.int32, (1, LANES), 1)
        both = jnp.where(lane == 0, latest, jnp.where(lane == 1, earlier, 0.0))
        sums_ref[...] = jnp.broadcast_to(both[None], (count, 1, LANES))
    else:
        pack_rows(next_ref, 1, send_ref, outs[1:3], outs[3])


def blocks_out_kernel(scaled_ref, index_ref, table_ref, side_ref, *refs):
    received, out_ref = refs[:RECEIVED], refs[RECEIVED]
    slots = out_ref.shape[1]
    for block in range(4):
        for first in range(0, slots, 8):
            count = min(8, slots - first)
            tile = slice(first, first + 8)
            index = index_ref[tile, lanes(block)]
            low, high = index & (LANES - 1), index >> 7
            for m in range(6):
                found = []
                for c in range(3):
                    row = slice(c * 8 + m, c * 8 + m + 1)
                    sources = [spread(table_ref[row, lanes(group)]) for group in range(4)]
                    found.append(pick(sources + ghost_rows(received, side_ref, row), low, high))
                for r in range(3):
                    total = None
                    for c in range(3):
                        term = scaled_ref[r * 3 + c, tile, lanes(block)] * found[c]
                        total = term if total is None else total + term
                    out_ref[r * 6 + m, first : first + count, lanes(block)] = total[0:count, :]


def regroup_kernel(sums_ref, out_ref):
    total = jnp.sum(sums_ref[...], axis=0, keepdims=True)
    out_ref[...] = jnp.broadcast_to(total, out_ref.shape)


def finish_kernel(sums_ref, raw_ref, table_ref, off_ref, self_ref, rho_ref):
    total = jnp.sum(sums_ref[...], axis=0)
    lane = lax.broadcasted_iota(jnp.int32, (1, LANES), 1)
    latest = jnp.sum(jnp.where(lane == 0, total, 0.0), keepdims=True)
    earlier = jnp.sum(jnp.where(lane == 1, total, 0.0), keepdims=True)
    rho = jnp.sqrt(latest / (earlier + 1e-05))
    rho_ref[...] = jnp.broadcast_to(rho, rho_ref.shape)
    factor = -(OMEGA / rho)
    for entry in range(raw_ref.shape[0]):
        off_ref[entry] = (factor * raw_ref[entry]).astype(jnp.bfloat16)
    keep = 1.0 - OMEGA / rho
    for row in range(3):
        self_ref[row * 6 : row * 6 + 6, :] = (keep * table_ref[row * 8 : row * 8 + 6, :]).astype(
            jnp.bfloat16
        )


def call(kernel, outs, *args):
    return pl.pallas_call(
        kernel,
        out_shape=[
            jax.ShapeDtypeStruct(*out) if len(out) == 2 else pltpu.VMEM(*out[:2]) for out in outs
        ],
        in_specs=[VM] * len(args),
        out_specs=[VM] * len(outs),
        compiler_params=pltpu.CompilerParams(vmem_limit_bytes=16 << 20),
    )(*args)


def far(array):
    return pltpu.with_memory_space_constraint(array, pltpu.HBM)


def kept(array):
    return pltpu.with_memory_space_constraint(array, pltpu.VMEM)


def swap(count, offset):
    pairs = []
    for i in range(offset, count - 1, 2):
        pairs += [(i, i + 1), (i + 1, i)]
    return pairs


def squares():
    slabs, subs = lax.axis_size("slab"), lax.axis_size(SUB)
    return [
        [(i + p) * subs + j + q for p in (0, 1) for q in (0, 1)]
        for i in range(0, slabs, 2)
        for j in range(0, subs, 2)
    ]


def exchange(a, b, both):
    subs, slabs = lax.axis_size(SUB), lax.axis_size("slab")
    ao = lax.ppermute(a, SUB, swap(subs, 1))
    bo = lax.ppermute(b, "slab", swap(slabs, 1))
    if MODE == "square":
        return ao, bo, lax.all_gather(both, SLAB_SUB, axis_index_groups=squares())
    be = lax.ppermute(b, "slab", swap(slabs, 0))
    if MODE == "core":
        return ao, be, bo, lax.all_gather(a, "sub_2")
    ae = lax.ppermute(a, SUB, swap(subs, 0))
    return ae, ao, be, bo


def body(near_null, aggregates, diag_block, off_blocks, columns, sends, start_vector):
    nodes = near_null.shape[1]
    slots = off_blocks.shape[0]
    padded = (slots + 7) // 8 * 8
    subs, slabs = lax.axis_size(SUB), lax.axis_size("slab")
    lane = jnp.arange(LANES, dtype=jnp.int32)[None, :]
    position = jnp.stack([lax.axis_index(SUB), lax.axis_index("slab")])[:, None] % 2
    side = ((lane < 64) == (position == 0)).astype(jnp.int32)
    side = jnp.concatenate([side, jnp.broadcast_to(position, side.shape)]).astype(jnp.int32)

    kept_f32 = lambda *shape: (shape, F32, "kept")
    kept_i32 = lambda *shape: (shape, jnp.int32, "kept")
    table, w, send, a, b, both = call(
        start_kernel,
        [kept_f32(24, nodes), kept_f32(8, nodes), kept_i32(2, LANES)]
        + [kept_f32(24, LANES)] * 2
        + [kept_f32(48, LANES)],
        far(near_null),
        far(aggregates[None, :]),
        far(start_vector),
        far(sends),
    )
    received = [kept(x) for x in exchange(a, b, both)]
    side = kept(side)
    scaled, index = call(
        blocks_kernel,
        [kept_f32(9, padded, nodes), kept_i32(padded, nodes)],
        far(diag_block),
        far(jnp.transpose(off_blocks, (1, 0, 2))),
        far(columns),
    )
    first_received = received
    for iteration in range(ITERS):
        last = iteration == ITERS - 1
        outs = [kept_f32(8, nodes)]
        outs += [kept_f32(subs, 1, LANES)] if last else [kept_f32(8, LANES)] * 2 + [kept_f32(16, LANES)]
        result = call(
            functools.partial(step_kernel, iteration == 0, last, subs),
            outs,
            kept(scaled),
            kept(index),
            kept(w),
            side,
            kept(send),
            *received,
        )
        w = result[0]
        if last:
            sums = result[1]
        else:
            received = [kept(x) for x in exchange(*result[1:])]
    (raw,) = call(
        blocks_out_kernel,
        [kept_f32(18, slots, nodes)],
        kept(scaled),
        kept(index),
        kept(table),
        side,
        *first_received,
    )
    sums = lax.all_to_all(sums, SUB, 0, 0, tiled=True)
    (sums,) = call(regroup_kernel, [kept_f32(slabs, 1, LANES)], kept(sums))
    sums = lax.all_to_all(sums, "slab", 0, 0, tiled=True)
    prolong_off, prolong_self, rho = call(
        finish_kernel,
        [((18, slots, nodes), jnp.bfloat16), ((18, nodes), jnp.bfloat16), ((1, LANES), F32)],
        kept(sums),
        kept(raw),
        kept(table),
    )
    return (jnp.transpose(prolong_off, (1, 0, 2)), prolong_self, rho[0, 0])


def solution(mesh):
    torus = Mesh(
        mesh.devices.reshape(mesh.shape["slab"], 8, 4, 2), ("slab", "sub_0", "sub_1", "sub_2")
    )
    placed = (
        P(None, SLAB_SUB),
        P(SLAB_SUB),
        P(None, SLAB_SUB),
        P(None, None, SLAB_SUB),
        P(None, SLAB_SUB),
        P(None, SLAB_SUB),
        P(None, SLAB_SUB),
    )
    return jax.shard_map(
        body,
        mesh=torus,
        in_specs=placed,
        out_specs=(P(None, None, SLAB_SUB), P(None, SLAB_SUB), P()),
        check_vma=False,
    )
```

```python
import functools

import jax
import jax.numpy as jnp
from jax import lax
from jax.experimental import pallas as pl
from jax.experimental.pallas import tpu as pltpu
from jax.sharding import Mesh
from jax.sharding import PartitionSpec as P

ITERS = 8
OMEGA = 4.0 / 3.0
SUB = ("sub_0", "sub_1", "sub_2")
SLAB_SUB = ("slab", "sub_0", "sub_1", "sub_2")
LANES = 128
F32 = jnp.float32
RECEIVED = 3
VM = pl.BlockSpec(memory_space=pltpu.VMEM)
HB = pl.BlockSpec(memory_space=pltpu.HBM)


def lanes(group):
    return slice(group * LANES, (group + 1) * LANES)


def pick(sources, low, high):
    result = jnp.take_along_axis(sources[0], low, axis=1, mode="promise_in_bounds")
    for group in range(1, len(sources)):
        found = jnp.take_along_axis(sources[group], low, axis=1, mode="promise_in_bounds")
        result = jnp.where(high == group, found, result)
    return result


def spread(row):
    return jnp.broadcast_to(row, (8, LANES))


def pack_rows(table_ref, tiles, send_ref, pay_refs, both_ref):
    for pay_ref, first in zip(pay_refs, (0, 1)):
        index = spread(send_ref[first : first + 1, :])
        low, high = index & (LANES - 1), index >> 7
        for tile in range(tiles):
            rows = slice(tile * 8, tile * 8 + 8)
            sources = [table_ref[rows, lanes(group)] for group in range(4)]
            pay_ref[rows, :] = pick(sources, low, high)
    both_ref[0 : tiles * 8, :] = pay_refs[0][...]
    both_ref[tiles * 8 :, :] = pay_refs[1][...]


def start_kernel(*refs):
    far_refs, refs = refs[:7], refs[7:]
    table_ref, w_ref, send_ref, a_ref, b_ref, both_ref, scaled_ref, index_ref = refs[:8]
    near_refs, sems = refs[8:15], refs[15:]
    copies = [
        pltpu.make_async_copy(source, target, sem)
        for source, target, sem in zip(far_refs, near_refs, sems)
    ]
    for copy in copies:
        copy.start()
    near_ref, aggregates_ref, start_ref, sends_ref, diag_ref, off_ref, columns_ref = near_refs
    for copy in copies[:4]:
        copy.wait()
    nodes = near_ref.shape[1]
    groups = nodes // 8
    for e in range(4):
        send_ref[e // 2 : e // 2 + 1, (e % 2) * 64 : (e % 2) * 64 + 64] = sends_ref[e : e + 1, :]
    name = lax.broadcasted_iota(jnp.int32, (groups, nodes), 0)
    members = (name == aggregates_ref[...]).astype(F32)
    sizes = jnp.sum(members, axis=1, keepdims=True)
    scale = lax.rsqrt(jnp.sum(members * sizes, axis=0, keepdims=True))
    table_ref[...] = jnp.zeros(table_ref.shape, F32)
    w_ref[...] = jnp.zeros(w_ref.shape, F32)
    for row in range(3):
        table_ref[row * 8 : row * 8 + 6, :] = near_ref[row * 6 : row * 6 + 6, :] * scale
        table_ref[row * 8 + 6 : row * 8 + 7, :] = start_ref[row : row + 1, :]
    w_ref[0:3, :] = start_ref[...]
    pack_rows(table_ref, 3, send_ref, (a_ref, b_ref), both_ref)
    for copy in copies[4:]:
        copy.wait()
    slots = off_ref.shape[1]
    index_ref[0:slots, :] = columns_ref[...]
    index_ref[slots:, :] = jnp.zeros((index_ref.shape[0] - slots, index_ref.shape[1]), jnp.int32)
    scaled_ref[:, slots:, :] = jnp.zeros(
        (9, scaled_ref.shape[1] - slots, scaled_ref.shape[2]), F32
    )
    entries = [diag_ref[position : position + 1, :] for position in range(9)]
    cofactor = [
        entries[4] * entries[8] - entries[5] * entries[7],
        entries[5] * entries[6] - entries[3] * entries[8],
        entries[3] * entries[7] - entries[4] * entries[6],
        entries[2] * entries[7] - entries[1] * entries[8],
        entries[0] * entries[8] - entries[2] * entries[6],
        entries[1] * entries[6] - entries[0] * entries[7],
        entries[1] * entries[5] - entries[2] * entries[4],
        entries[2] * entries[3] - entries[0] * entries[5],
        entries[0] * entries[4] - entries[1] * entries[3],
    ]
    determinant = entries[0] * cofactor[0] + entries[1] * cofactor[1] + entries[2] * cofactor[2]
    inverse = [
        [cofactor[column * 3 + row] / determinant for column in range(3)] for row in range(3)
    ]
    for column in range(3):
        block = [off_ref[inner * 3 + column] for inner in range(3)]
        for row in range(3):
            total = inverse[row][0] * block[0]
            total = total + inverse[row][1] * block[1]
            total = total + inverse[row][2] * block[2]
            scaled_ref[row * 3 + column, 0:slots, :] = total


def ghost_rows(refs, side_ref, row):
    ao, bo, gathered = refs
    odd_sub = side_ref[2:3, :] != 0
    odd_slab = side_ref[3:4, :] != 0
    half = gathered.shape[1] // 2
    down = slice(row.start + half, row.stop + half)
    even_a = jnp.where(
        odd_slab,
        jnp.where(odd_sub, gathered[2, row, :], gathered[3, row, :]),
        jnp.where(odd_sub, gathered[0, row, :], gathered[1, row, :]),
    )
    even_b = jnp.where(
        odd_slab,
        jnp.where(odd_sub, gathered[1, down, :], gathered[0, down, :]),
        jnp.where(odd_sub, gathered[3, down, :], gathered[2, down, :]),
    )
    return [
        spread(jnp.where(side_ref[0:1, :] != 0, ao[row, :], even_a)),
        spread(jnp.where(side_ref[1:2, :] != 0, bo[row, :], even_b)),
    ]


def step_kernel(first, last, *refs):
    scaled_ref, index_ref, w_ref, side_ref, send_ref = refs[:5]
    received = refs[5 : 5 + RECEIVED]
    outs = refs[5 + RECEIVED :]
    table = []
    for c in range(3):
        row = c * 8 + 6 if first else c
        table.append(
            [spread(w_ref[c : c + 1, lanes(group)]) for group in range(4)]
            + ghost_rows(received, side_ref, slice(row, row + 1))
        )
    if not last:
        outs[0][...] = jnp.zeros(outs[0].shape, F32)
    latest = jnp.zeros((1, LANES), F32)
    for block in range(4):
        total = [None] * 3
        for tile in range(4):
            slots = slice(tile * 8, tile * 8 + 8)
            index = index_ref[slots, lanes(block)]
            low, high = index & (LANES - 1), index >> 7
            for c in range(3):
                found = pick(table[c], low, high)
                for r in range(3):
                    term = scaled_ref[r * 3 + c, slots, lanes(block)] * found
                    total[r] = term if total[r] is None else total[r] + term
        for r in range(3):
            new = w_ref[r : r + 1, lanes(block)] + jnp.sum(total[r], axis=0, keepdims=True)
            if last:
                latest = latest + new * new
            else:
                outs[0][r : r + 1, lanes(block)] = new
    if last:
        (sums_ref,) = outs
        earlier = jnp.zeros((8, LANES), F32)
        for block in range(4):
            old = w_ref[:, lanes(block)]
            earlier = earlier + old * old
        earlier = jnp.sum(earlier, axis=0, keepdims=True)
        count = sums_ref.shape[0]
        latest = latest + pltpu.roll(latest, 64, 1)
        earlier = earlier + pltpu.roll(earlier, 64, 1)
        lane = lax.broadcasted_iota(jnp.int32, (1, LANES), 1)
        both = jnp.where(lane < 64, latest, earlier)
        sums_ref[...] = jnp.broadcast_to(both[None], (count, 1, LANES))
    else:
        pack_rows(outs[0], 1, send_ref, outs[1:3], outs[3])


def blocks_out_kernel(scaled_ref, index_ref, table_ref, side_ref, *refs):
    received, out_ref = refs[:RECEIVED], refs[RECEIVED]
    slots = out_ref.shape[1]
    for block in range(4):
        for first in range(0, slots, 8):
            count = min(8, slots - first)
            tile = slice(first, first + 8)
            index = index_ref[tile, lanes(block)]
            low, high = index & (LANES - 1), index >> 7
            for m in range(6):
                found = []
                for c in range(3):
                    row = slice(c * 8 + m, c * 8 + m + 1)
                    sources = [spread(table_ref[row, lanes(group)]) for group in range(4)]
                    found.append(pick(sources + ghost_rows(received, side_ref, row), low, high))
                for r in range(3):
                    total = None
                    for c in range(3):
                        term = scaled_ref[r * 3 + c, tile, lanes(block)] * found[c]
                        total = term if total is None else total + term
                    out_ref[r * 6 + m, first : first + count, lanes(block)] = total[0:count, :]


def regroup_kernel(sums_ref, out_ref):
    total = jnp.sum(sums_ref[...], axis=0, keepdims=True)
    out_ref[...] = jnp.broadcast_to(total, out_ref.shape)


def finish_kernel(sums_ref, raw_ref, table_ref, off_ref, self_ref, rho_ref):
    total = jnp.sum(sums_ref[...], axis=0)
    lane = lax.broadcasted_iota(jnp.int32, (1, LANES), 1)
    latest = jnp.sum(jnp.where(lane < 64, total, 0.0), axis=1, keepdims=True)
    earlier = jnp.sum(jnp.where(lane < 64, 0.0, total), axis=1, keepdims=True)
    rho = jnp.sqrt(latest / (earlier + 1e-05))
    rho_ref[...] = jnp.broadcast_to(rho, rho_ref.shape)
    factor = -(OMEGA / rho)
    for entry in range(raw_ref.shape[0]):
        off_ref[entry] = (factor * raw_ref[entry]).astype(jnp.bfloat16)
    keep = 1.0 - OMEGA / rho
    for row in range(3):
        self_ref[row * 6 : row * 6 + 6, :] = (keep * table_ref[row * 8 : row * 8 + 6, :]).astype(
            jnp.bfloat16
        )


def call(kernel, name, outs, *args, near=None, scratch=()):
    near = len(args) if near is None else near
    return pl.pallas_call(
        kernel,
        name=name,
        out_shape=[
            jax.ShapeDtypeStruct(*out) if len(out) == 2 else pltpu.VMEM(*out[:2]) for out in outs
        ],
        in_specs=[VM] * near + [HB] * (len(args) - near),
        out_specs=[VM] * len(outs),
        scratch_shapes=list(scratch),
        compiler_params=pltpu.CompilerParams(vmem_limit_bytes=16 << 20),
    )(*args)


def far(array):
    return pltpu.with_memory_space_constraint(array, pltpu.HBM)


def kept(array):
    return pltpu.with_memory_space_constraint(array, pltpu.VMEM)


def swap(count, offset):
    pairs = []
    for i in range(offset, count - 1, 2):
        pairs += [(i, i + 1), (i + 1, i)]
    return pairs


def squares():
    slabs, subs = lax.axis_size("slab"), lax.axis_size(SUB)
    return [
        [(i + p) * subs + j + q for p in (0, 1) for q in (0, 1)]
        for i in range(0, slabs, 2)
        for j in range(0, subs, 2)
    ]


def exchange(a, b, both):
    bo = lax.ppermute(b, "slab", swap(lax.axis_size("slab"), 1))
    ao = lax.ppermute(a, SUB, swap(lax.axis_size(SUB), 1))
    return ao, bo, lax.all_gather(both, SLAB_SUB, axis_index_groups=squares())


def body(near_null, aggregates, diag_block, off_blocks, columns, sends, start_vector):
    nodes = near_null.shape[1]
    slots = off_blocks.shape[0]
    padded = (slots + 7) // 8 * 8
    subs, slabs = lax.axis_size(SUB), lax.axis_size("slab")
    lane = jnp.arange(LANES, dtype=jnp.int32)[None, :]
    position = jnp.stack([lax.axis_index(SUB), lax.axis_index("slab")])[:, None] % 2
    side = ((lane < 64) == (position == 0)).astype(jnp.int32)
    side = jnp.concatenate([side, jnp.broadcast_to(position, side.shape)]).astype(jnp.int32)

    kept_f32 = lambda *shape: (shape, F32, "kept")
    kept_i32 = lambda *shape: (shape, jnp.int32, "kept")
    table, w, send, a, b, both, scaled, index = call(
        start_kernel,
        "start",
        [kept_f32(24, nodes), kept_f32(8, nodes), kept_i32(2, LANES)]
        + [kept_f32(24, LANES)] * 2
        + [kept_f32(48, LANES), kept_f32(9, padded, nodes), kept_i32(padded, nodes)],
        far(near_null),
        far(aggregates[None, :]),
        far(start_vector),
        far(sends),
        far(diag_block),
        far(jnp.transpose(off_blocks, (1, 0, 2))),
        far(columns),
        near=0,
        scratch=[
            pltpu.VMEM((18, nodes), F32),
            pltpu.VMEM((1, nodes), jnp.int32),
            pltpu.VMEM((3, nodes), F32),
            pltpu.VMEM((4, 64), jnp.int32),
            pltpu.VMEM((9, nodes), F32),
            pltpu.VMEM((9, slots, nodes), F32),
            pltpu.VMEM((slots, nodes), jnp.int32),
        ]
        + [pltpu.SemaphoreType.DMA] * 7,
    )
    received = [kept(x) for x in exchange(a, b, both)]
    side = kept(side)
    first_received = received
    for iteration in range(ITERS):
        last = iteration == ITERS - 1
        outs = [kept_f32(8, nodes)] + [kept_f32(8, LANES)] * 2 + [kept_f32(16, LANES)]
        if last:
            outs = [kept_f32(subs, 1, LANES)]
        result = call(
            functools.partial(step_kernel, iteration == 0, last),
            f"step_{iteration}",
            outs,
            kept(scaled),
            kept(index),
            kept(w),
            side,
            kept(send),
            *received,
        )
        if last:
            (sums,) = result
        else:
            w = result[0]
            received = [kept(x) for x in exchange(*result[1:])]
    (raw,) = call(
        blocks_out_kernel,
        "blocks_out",
        [kept_f32(18, slots, nodes)],
        kept(scaled),
        kept(index),
        kept(table),
        side,
        *first_received,
    )
    sums = lax.all_to_all(sums, SUB, 0, 0, tiled=True)
    (sums,) = call(regroup_kernel, "regroup", [kept_f32(slabs, 1, LANES)], kept(sums))
    sums = lax.all_to_all(sums, "slab", 0, 0, tiled=True)
    prolong_off, prolong_self, rho = call(
        finish_kernel,
        "finish",
        [((18, slots, nodes), jnp.bfloat16), ((18, nodes), jnp.bfloat16), ((1, LANES), F32)],
        kept(sums),
        kept(raw),
        kept(table),
    )
    return (jnp.transpose(prolong_off, (1, 0, 2)), prolong_self, rho[0, 0])


def solution(mesh):
    torus = Mesh(
        mesh.devices.reshape(mesh.shape["slab"], 8, 4, 2), ("slab", "sub_0", "sub_1", "sub_2")
    )
    placed = (
        P(None, SLAB_SUB),
        P(SLAB_SUB),
        P(None, SLAB_SUB),
        P(None, None, SLAB_SUB),
        P(None, SLAB_SUB),
        P(None, SLAB_SUB),
        P(None, SLAB_SUB),
    )
    return jax.shard_map(
        body,
        mesh=torus,
        in_specs=placed,
        out_specs=(P(None, None, SLAB_SUB), P(None, SLAB_SUB), P()),
        check_vma=False,
    )
```

```python
import functools

import jax
import jax.numpy as jnp
from jax import lax
from jax.experimental import pallas as pl
from jax.experimental.pallas import tpu as pltpu
from jax.sharding import Mesh
from jax.sharding import PartitionSpec as P

ITERS = 8
OMEGA = 4.0 / 3.0
SUB = ("sub_0", "sub_1", "sub_2")
FIRST = ("slab", "sub_2")
SECOND = ("sub_0", "sub_1")
SLAB_SUB = ("slab", "sub_0", "sub_1", "sub_2")
LANES = 128
F32 = jnp.float32
RECEIVED = 3
VM = pl.BlockSpec(memory_space=pltpu.VMEM)
HB = pl.BlockSpec(memory_space=pltpu.HBM)


def lanes(group):
    return slice(group * LANES, (group + 1) * LANES)


def pick(sources, low, high):
    result = jnp.take_along_axis(sources[0], low, axis=1, mode="promise_in_bounds")
    for group in range(1, len(sources)):
        found = jnp.take_along_axis(sources[group], low, axis=1, mode="promise_in_bounds")
        result = jnp.where(high == group, found, result)
    return result


def spread(row):
    return jnp.broadcast_to(row, (8, LANES))


def pack_rows(table_ref, tiles, send_ref, pay_refs, both_ref):
    for pay_ref, first in zip(pay_refs, (0, 1)):
        index = spread(send_ref[first : first + 1, :])
        low, high = index & (LANES - 1), index >> 7
        for tile in range(tiles):
            rows = slice(tile * 8, tile * 8 + 8)
            sources = [table_ref[rows, lanes(group)] for group in range(4)]
            pay_ref[rows, :] = pick(sources, low, high)
    rows = 3 if tiles == 1 else tiles * 8
    if tiles == 1:
        both_ref[...] = jnp.zeros(both_ref.shape, F32)
    both_ref[0:rows, :] = pay_refs[0][0:rows, :]
    both_ref[rows : 2 * rows, :] = pay_refs[1][0:rows, :]


def start_kernel(*refs):
    far_refs, refs = refs[:7], refs[7:]
    table_ref, w_ref, send_ref, a_ref, b_ref, both_ref, scaled_ref, index_ref = refs[:8]
    near_refs, sems = refs[8:15], refs[15:]
    copies = [
        pltpu.make_async_copy(source, target, sem)
        for source, target, sem in zip(far_refs, near_refs, sems)
    ]
    for copy in copies:
        copy.start()
    near_ref, aggregates_ref, start_ref, sends_ref, diag_ref, off_ref, columns_ref = near_refs
    for copy in copies[:4]:
        copy.wait()
    nodes = near_ref.shape[1]
    groups = nodes // 8
    for e in range(4):
        send_ref[e // 2 : e // 2 + 1, (e % 2) * 64 : (e % 2) * 64 + 64] = sends_ref[e : e + 1, :]
    name = lax.broadcasted_iota(jnp.int32, (groups, nodes), 0)
    members = (name == aggregates_ref[...]).astype(F32)
    sizes = jnp.sum(members, axis=1, keepdims=True)
    scale = lax.rsqrt(jnp.sum(members * sizes, axis=0, keepdims=True))
    table_ref[...] = jnp.zeros(table_ref.shape, F32)
    w_ref[...] = jnp.zeros(w_ref.shape, F32)
    for row in range(3):
        table_ref[row * 8 : row * 8 + 6, :] = near_ref[row * 6 : row * 6 + 6, :] * scale
        table_ref[row * 8 + 6 : row * 8 + 7, :] = start_ref[row : row + 1, :]
    w_ref[0:3, :] = start_ref[...]
    pack_rows(table_ref, 3, send_ref, (a_ref, b_ref), both_ref)
    for copy in copies[4:]:
        copy.wait()
    slots = off_ref.shape[1]
    index_ref[0:slots, :] = columns_ref[...]
    index_ref[slots:, :] = jnp.zeros((index_ref.shape[0] - slots, index_ref.shape[1]), jnp.int32)
    scaled_ref[:, slots:, :] = jnp.zeros(
        (9, scaled_ref.shape[1] - slots, scaled_ref.shape[2]), F32
    )
    entries = [diag_ref[position : position + 1, :] for position in range(9)]
    cofactor = [
        entries[4] * entries[8] - entries[5] * entries[7],
        entries[5] * entries[6] - entries[3] * entries[8],
        entries[3] * entries[7] - entries[4] * entries[6],
        entries[2] * entries[7] - entries[1] * entries[8],
        entries[0] * entries[8] - entries[2] * entries[6],
        entries[1] * entries[6] - entries[0] * entries[7],
        entries[1] * entries[5] - entries[2] * entries[4],
        entries[2] * entries[3] - entries[0] * entries[5],
        entries[0] * entries[4] - entries[1] * entries[3],
    ]
    determinant = entries[0] * cofactor[0] + entries[1] * cofactor[1] + entries[2] * cofactor[2]
    inverse = [
        [cofactor[column * 3 + row] / determinant for column in range(3)] for row in range(3)
    ]
    for column in range(3):
        block = [off_ref[inner * 3 + column] for inner in range(3)]
        for row in range(3):
            total = inverse[row][0] * block[0]
            total = total + inverse[row][1] * block[1]
            total = total + inverse[row][2] * block[2]
            scaled_ref[row * 3 + column, 0:slots, :] = total


def ghost_rows(refs, side_ref, row):
    ao, bo, gathered = refs
    odd_sub = side_ref[2:3, :] != 0
    odd_slab = side_ref[3:4, :] != 0
    half = 3 if gathered.shape[1] == 8 else gathered.shape[1] // 2
    down = slice(row.start + half, row.stop + half)
    even_a = jnp.where(
        odd_slab,
        jnp.where(odd_sub, gathered[2, row, :], gathered[3, row, :]),
        jnp.where(odd_sub, gathered[0, row, :], gathered[1, row, :]),
    )
    even_b = jnp.where(
        odd_slab,
        jnp.where(odd_sub, gathered[1, down, :], gathered[0, down, :]),
        jnp.where(odd_sub, gathered[3, down, :], gathered[2, down, :]),
    )
    return [
        spread(jnp.where(side_ref[0:1, :] != 0, ao[row, :], even_a)),
        spread(jnp.where(side_ref[1:2, :] != 0, bo[row, :], even_b)),
    ]


def step_kernel(first, last, *refs):
    scaled_ref, index_ref, w_ref, side_ref, send_ref = refs[:5]
    received = refs[5 : 5 + RECEIVED]
    outs = refs[5 + RECEIVED :]
    table = []
    for c in range(3):
        row = c * 8 + 6 if first else c
        table.append(
            [spread(w_ref[c : c + 1, lanes(group)]) for group in range(4)]
            + ghost_rows(received, side_ref, slice(row, row + 1))
        )
    if not last:
        outs[0][...] = jnp.zeros(outs[0].shape, F32)
    latest = jnp.zeros((1, LANES), F32)
    for block in range(4):
        total = [None] * 3
        for tile in range(4):
            slots = slice(tile * 8, tile * 8 + 8)
            index = index_ref[slots, lanes(block)]
            low, high = index & (LANES - 1), index >> 7
            for c in range(3):
                found = pick(table[c], low, high)
                for r in range(3):
                    term = scaled_ref[r * 3 + c, slots, lanes(block)] * found
                    total[r] = term if total[r] is None else total[r] + term
        for r in range(3):
            new = w_ref[r : r + 1, lanes(block)] + jnp.sum(total[r], axis=0, keepdims=True)
            if last:
                latest = latest + new * new
            else:
                outs[0][r : r + 1, lanes(block)] = new
    if last:
        (sums_ref,) = outs
        earlier = jnp.zeros((8, LANES), F32)
        for block in range(4):
            old = w_ref[:, lanes(block)]
            earlier = earlier + old * old
        earlier = jnp.sum(earlier, axis=0, keepdims=True)
        count = sums_ref.shape[0]
        latest = latest + pltpu.roll(latest, 64, 1)
        earlier = earlier + pltpu.roll(earlier, 64, 1)
        lane = lax.broadcasted_iota(jnp.int32, (1, LANES), 1)
        both = jnp.where(lane < 64, latest, earlier)
        sums_ref[...] = jnp.broadcast_to(both[None], (count, 1, LANES))
    else:
        pack_rows(outs[0], 1, send_ref, outs[1:3], outs[3])


def blocks_out_kernel(scaled_ref, index_ref, table_ref, side_ref, *refs):
    received, out_ref = refs[:RECEIVED], refs[RECEIVED]
    slots = out_ref.shape[1]
    for block in range(4):
        for first in range(0, slots, 8):
            count = min(8, slots - first)
            tile = slice(first, first + 8)
            index = index_ref[tile, lanes(block)]
            low, high = index & (LANES - 1), index >> 7
            for m in range(6):
                found = []
                for c in range(3):
                    row = slice(c * 8 + m, c * 8 + m + 1)
                    sources = [spread(table_ref[row, lanes(group)]) for group in range(4)]
                    found.append(pick(sources + ghost_rows(received, side_ref, row), low, high))
                for r in range(3):
                    total = None
                    for c in range(3):
                        term = scaled_ref[r * 3 + c, tile, lanes(block)] * found[c]
                        total = term if total is None else total + term
                    out_ref[r * 6 + m, first : first + count, lanes(block)] = total[0:count, :]


def regroup_kernel(sums_ref, out_ref):
    total = jnp.sum(sums_ref[...], axis=0, keepdims=True)
    out_ref[...] = jnp.broadcast_to(total, out_ref.shape)


def finish_kernel(sums_ref, raw_ref, table_ref, off_ref, self_ref, rho_ref):
    total = jnp.sum(sums_ref[...], axis=0)
    lane = lax.broadcasted_iota(jnp.int32, (1, LANES), 1)
    latest = jnp.sum(jnp.where(lane < 64, total, 0.0), axis=1, keepdims=True)
    earlier = jnp.sum(jnp.where(lane < 64, 0.0, total), axis=1, keepdims=True)
    rho = jnp.sqrt(latest / (earlier + 1e-05))
    rho_ref[...] = jnp.broadcast_to(rho, rho_ref.shape)
    factor = -(OMEGA / rho)
    for entry in range(raw_ref.shape[0]):
        off_ref[entry] = (factor * raw_ref[entry]).astype(jnp.bfloat16)
    keep = 1.0 - OMEGA / rho
    for row in range(3):
        self_ref[row * 6 : row * 6 + 6, :] = (keep * table_ref[row * 8 : row * 8 + 6, :]).astype(
            jnp.bfloat16
        )


def call(kernel, name, outs, *args, near=None, scratch=()):
    near = len(args) if near is None else near
    return pl.pallas_call(
        kernel,
        name=name,
        out_shape=[
            jax.ShapeDtypeStruct(*out) if len(out) == 2 else pltpu.VMEM(*out[:2]) for out in outs
        ],
        in_specs=[VM] * near + [HB] * (len(args) - near),
        out_specs=[VM] * len(outs),
        scratch_shapes=list(scratch),
        compiler_params=pltpu.CompilerParams(vmem_limit_bytes=16 << 20),
    )(*args)


def far(array):
    return pltpu.with_memory_space_constraint(array, pltpu.HBM)


def kept(array):
    return pltpu.with_memory_space_constraint(array, pltpu.VMEM)


def swap(count, offset):
    pairs = []
    for i in range(offset, count - 1, 2):
        pairs += [(i, i + 1), (i + 1, i)]
    return pairs


def squares():
    slabs, subs = lax.axis_size("slab"), lax.axis_size(SUB)
    return [
        [(i + p) * subs + j + q for p in (0, 1) for q in (0, 1)]
        for i in range(0, slabs, 2)
        for j in range(0, subs, 2)
    ]


def exchange(a, b, both):
    bo = lax.ppermute(b, "slab", swap(lax.axis_size("slab"), 1))
    ao = lax.ppermute(a, SUB, swap(lax.axis_size(SUB), 1))
    return ao, bo, lax.all_gather(both, SLAB_SUB, axis_index_groups=squares())


def body(near_null, aggregates, diag_block, off_blocks, columns, sends, start_vector):
    nodes = near_null.shape[1]
    slots = off_blocks.shape[0]
    padded = (slots + 7) // 8 * 8
    subs, slabs = lax.axis_size(SUB), lax.axis_size("slab")
    lane = jnp.arange(LANES, dtype=jnp.int32)[None, :]
    position = jnp.stack([lax.axis_index(SUB), lax.axis_index("slab")])[:, None] % 2
    side = ((lane < 64) == (position == 0)).astype(jnp.int32)
    side = jnp.concatenate([side, jnp.broadcast_to(position, side.shape)]).astype(jnp.int32)

    kept_f32 = lambda *shape: (shape, F32, "kept")
    kept_i32 = lambda *shape: (shape, jnp.int32, "kept")
    table, w, send, a, b, both, scaled, index = call(
        start_kernel,
        "start",
        [kept_f32(24, nodes), kept_f32(8, nodes), kept_i32(2, LANES)]
        + [kept_f32(24, LANES)] * 2
        + [kept_f32(48, LANES), kept_f32(9, padded, nodes), kept_i32(padded, nodes)],
        far(near_null),
        far(aggregates[None, :]),
        far(start_vector),
        far(sends),
        far(diag_block),
        far(jnp.transpose(off_blocks, (1, 0, 2))),
        far(columns),
        near=0,
        scratch=[
            pltpu.VMEM((18, nodes), F32),
            pltpu.VMEM((1, nodes), jnp.int32),
            pltpu.VMEM((3, nodes), F32),
            pltpu.VMEM((4, 64), jnp.int32),
            pltpu.VMEM((9, nodes), F32),
            pltpu.VMEM((9, slots, nodes), F32),
            pltpu.VMEM((slots, nodes), jnp.int32),
        ]
        + [pltpu.SemaphoreType.DMA] * 7,
    )
    received = [kept(x) for x in exchange(a, b, both)]
    side = kept(side)
    first_received = received
    for iteration in range(ITERS):
        last = iteration == ITERS - 1
        outs = [kept_f32(8, nodes)] + [kept_f32(8, LANES)] * 3
        if last:
            outs = [kept_f32(lax.axis_size(FIRST), 1, LANES)]
        result = call(
            functools.partial(step_kernel, iteration == 0, last),
            f"step_{iteration}",
            outs,
            kept(scaled),
            kept(index),
            kept(w),
            side,
            kept(send),
            *received,
        )
        if last:
            (sums,) = result
        else:
            w = result[0]
            received = [kept(x) for x in exchange(*result[1:])]
    (raw,) = call(
        blocks_out_kernel,
        "blocks_out",
        [kept_f32(18, slots, nodes)],
        kept(scaled),
        kept(index),
        kept(table),
        side,
        *first_received,
    )
    sums = lax.all_to_all(sums, FIRST, 0, 0, tiled=True)
    (sums,) = call(regroup_kernel, "regroup", [kept_f32(lax.axis_size(SECOND), 1, LANES)], kept(sums))
    sums = lax.all_to_all(sums, SECOND, 0, 0, tiled=True)
    prolong_off, prolong_self, rho = call(
        finish_kernel,
        "finish",
        [((18, slots, nodes), jnp.bfloat16), ((18, nodes), jnp.bfloat16), ((1, LANES), F32)],
        kept(sums),
        kept(raw),
        kept(table),
    )
    return (jnp.transpose(prolong_off, (1, 0, 2)), prolong_self, rho[0, 0])


def solution(mesh):
    torus = Mesh(
        mesh.devices.reshape(mesh.shape["slab"], 8, 4, 2), ("slab", "sub_0", "sub_1", "sub_2")
    )
    placed = (
        P(None, SLAB_SUB),
        P(SLAB_SUB),
        P(None, SLAB_SUB),
        P(None, None, SLAB_SUB),
        P(None, SLAB_SUB),
        P(None, SLAB_SUB),
        P(None, SLAB_SUB),
    )
    return jax.shard_map(
        body,
        mesh=torus,
        in_specs=placed,
        out_specs=(P(None, None, SLAB_SUB), P(None, SLAB_SUB), P()),
        check_vma=False,
    )
```

```python
import functools

import jax
import jax.numpy as jnp
from jax import lax
from jax.experimental import pallas as pl
from jax.experimental.pallas import tpu as pltpu
from jax.sharding import Mesh
from jax.sharding import PartitionSpec as P

ITERS = 8
OMEGA = 4.0 / 3.0
SUB = ("sub_0", "sub_1", "sub_2")
FIRST = ("slab", "sub_2")
SECOND = ("sub_0", "sub_1")
SLAB_SUB = ("slab", "sub_0", "sub_1", "sub_2")
LANES = 128
F32 = jnp.float32
RECEIVED = 3
VM = pl.BlockSpec(memory_space=pltpu.VMEM)
HB = pl.BlockSpec(memory_space=pltpu.HBM)


def lanes(group):
    return slice(group * LANES, (group + 1) * LANES)


def pick(sources, low, high):
    result = jnp.take_along_axis(sources[0], low, axis=1, mode="promise_in_bounds")
    for group in range(1, len(sources)):
        found = jnp.take_along_axis(sources[group], low, axis=1, mode="promise_in_bounds")
        result = jnp.where(high == group, found, result)
    return result


def spread(row):
    return jnp.broadcast_to(row, (8, LANES))


def pack_rows(table_ref, tiles, send_ref, pay_refs, both_ref):
    for pay_ref, first in zip(pay_refs, (0, 1)):
        index = spread(send_ref[first : first + 1, :])
        low, high = index & (LANES - 1), index >> 7
        for tile in range(tiles):
            rows = slice(tile * 8, tile * 8 + 8)
            sources = [table_ref[rows, lanes(group)] for group in range(4)]
            pay_ref[rows, :] = pick(sources, low, high)
    rows = 3 if tiles == 1 else tiles * 8
    if tiles == 1:
        both_ref[...] = jnp.zeros(both_ref.shape, F32)
    both_ref[0:rows, :] = pay_refs[0][0:rows, :]
    both_ref[rows : 2 * rows, :] = pay_refs[1][0:rows, :]


def start_kernel(*refs):
    far_refs, refs = refs[:7], refs[7:]
    table_ref, w_ref, send_ref, a_ref, b_ref, both_ref, scaled_ref, index_ref, side_ref = refs[:9]
    near_refs, sems = refs[9:16], refs[16:]
    copies = [
        pltpu.make_async_copy(source, target, sem)
        for source, target, sem in zip(far_refs, near_refs, sems)
    ]
    for copy in copies:
        copy.start()
    near_ref, aggregates_ref, start_ref, sends_ref, diag_ref, off_ref, columns_ref = near_refs
    lane = lax.broadcasted_iota(jnp.int32, (1, LANES), 1)
    low_half = (lane < 64).astype(jnp.int32)
    for row, axis in enumerate((SUB, "slab")):
        odd = (lane * 0 + lax.axis_index(axis)) & 1
        side_ref[row : row + 1, :] = low_half ^ odd
        side_ref[row + 2 : row + 3, :] = odd
    for copy in copies[:4]:
        copy.wait()
    nodes = near_ref.shape[1]
    groups = nodes // 8
    for e in range(4):
        send_ref[e // 2 : e // 2 + 1, (e % 2) * 64 : (e % 2) * 64 + 64] = sends_ref[e : e + 1, :]
    name = lax.broadcasted_iota(jnp.int32, (groups, nodes), 0)
    members = (name == aggregates_ref[...]).astype(F32)
    sizes = jnp.sum(members, axis=1, keepdims=True)
    scale = lax.rsqrt(jnp.sum(members * sizes, axis=0, keepdims=True))
    table_ref[...] = jnp.zeros(table_ref.shape, F32)
    w_ref[...] = jnp.zeros(w_ref.shape, F32)
    for row in range(3):
        table_ref[row * 8 : row * 8 + 6, :] = near_ref[row * 6 : row * 6 + 6, :] * scale
        table_ref[row * 8 + 6 : row * 8 + 7, :] = start_ref[row : row + 1, :]
    w_ref[0:3, :] = start_ref[...]
    pack_rows(table_ref, 3, send_ref, (a_ref, b_ref), both_ref)
    for copy in copies[4:]:
        copy.wait()
    slots = off_ref.shape[1]
    index_ref[0:slots, :] = columns_ref[...]
    index_ref[slots:, :] = jnp.zeros((index_ref.shape[0] - slots, index_ref.shape[1]), jnp.int32)
    scaled_ref[:, slots:, :] = jnp.zeros(
        (9, scaled_ref.shape[1] - slots, scaled_ref.shape[2]), F32
    )
    entries = [diag_ref[position : position + 1, :] for position in range(9)]
    cofactor = [
        entries[4] * entries[8] - entries[5] * entries[7],
        entries[5] * entries[6] - entries[3] * entries[8],
        entries[3] * entries[7] - entries[4] * entries[6],
        entries[2] * entries[7] - entries[1] * entries[8],
        entries[0] * entries[8] - entries[2] * entries[6],
        entries[1] * entries[6] - entries[0] * entries[7],
        entries[1] * entries[5] - entries[2] * entries[4],
        entries[2] * entries[3] - entries[0] * entries[5],
        entries[0] * entries[4] - entries[1] * entries[3],
    ]
    determinant = entries[0] * cofactor[0] + entries[1] * cofactor[1] + entries[2] * cofactor[2]
    inverse = [
        [cofactor[column * 3 + row] / determinant for column in range(3)] for row in range(3)
    ]
    for column in range(3):
        block = [off_ref[inner * 3 + column] for inner in range(3)]
        for row in range(3):
            total = inverse[row][0] * block[0]
            total = total + inverse[row][1] * block[1]
            total = total + inverse[row][2] * block[2]
            scaled_ref[row * 3 + column, 0:slots, :] = total


def ghost_rows(refs, side_ref, row):
    ao, bo, gathered = refs
    odd_sub = side_ref[2:3, :] != 0
    odd_slab = side_ref[3:4, :] != 0
    half = 3 if gathered.shape[1] == 8 else gathered.shape[1] // 2
    down = slice(row.start + half, row.stop + half)
    even_a = jnp.where(
        odd_slab,
        jnp.where(odd_sub, gathered[2, row, :], gathered[3, row, :]),
        jnp.where(odd_sub, gathered[0, row, :], gathered[1, row, :]),
    )
    even_b = jnp.where(
        odd_slab,
        jnp.where(odd_sub, gathered[1, down, :], gathered[0, down, :]),
        jnp.where(odd_sub, gathered[3, down, :], gathered[2, down, :]),
    )
    return [
        spread(jnp.where(side_ref[0:1, :] != 0, ao[row, :], even_a)),
        spread(jnp.where(side_ref[1:2, :] != 0, bo[row, :], even_b)),
    ]


def step_kernel(first, last, *refs):
    scaled_ref, index_ref, w_ref, side_ref, send_ref = refs[:5]
    received = refs[5 : 5 + RECEIVED]
    outs = refs[5 + RECEIVED :]
    table = []
    for c in range(3):
        row = c * 8 + 6 if first else c
        table.append(
            [spread(w_ref[c : c + 1, lanes(group)]) for group in range(4)]
            + ghost_rows(received, side_ref, slice(row, row + 1))
        )
    if not last:
        outs[0][...] = jnp.zeros(outs[0].shape, F32)
    latest = jnp.zeros((1, LANES), F32)
    for block in range(4):
        total = [None] * 3
        for tile in range(4):
            slots = slice(tile * 8, tile * 8 + 8)
            index = index_ref[slots, lanes(block)]
            low, high = index & (LANES - 1), index >> 7
            for c in range(3):
                found = pick(table[c], low, high)
                for r in range(3):
                    term = scaled_ref[r * 3 + c, slots, lanes(block)] * found
                    total[r] = term if total[r] is None else total[r] + term
        for r in range(3):
            new = w_ref[r : r + 1, lanes(block)] + jnp.sum(total[r], axis=0, keepdims=True)
            if last:
                latest = latest + new * new
            else:
                outs[0][r : r + 1, lanes(block)] = new
    if last:
        (sums_ref,) = outs
        earlier = jnp.zeros((8, LANES), F32)
        for block in range(4):
            old = w_ref[:, lanes(block)]
            earlier = earlier + old * old
        earlier = jnp.sum(earlier, axis=0, keepdims=True)
        count = sums_ref.shape[0]
        latest = latest + pltpu.roll(latest, 64, 1)
        earlier = earlier + pltpu.roll(earlier, 64, 1)
        lane = lax.broadcasted_iota(jnp.int32, (1, LANES), 1)
        both = jnp.where(lane < 64, latest, earlier)
        sums_ref[...] = jnp.broadcast_to(both[None], (count, 1, LANES))
    else:
        pack_rows(outs[0], 1, send_ref, outs[1:3], outs[3])


def blocks_out_kernel(scaled_ref, index_ref, table_ref, side_ref, *refs):
    received, out_ref = refs[:RECEIVED], refs[RECEIVED]
    slots = out_ref.shape[1]
    for block in range(4):
        for first in range(0, slots, 8):
            count = min(8, slots - first)
            tile = slice(first, first + 8)
            index = index_ref[tile, lanes(block)]
            low, high = index & (LANES - 1), index >> 7
            for m in range(6):
                found = []
                for c in range(3):
                    row = slice(c * 8 + m, c * 8 + m + 1)
                    sources = [spread(table_ref[row, lanes(group)]) for group in range(4)]
                    found.append(pick(sources + ghost_rows(received, side_ref, row), low, high))
                for r in range(3):
                    total = None
                    for c in range(3):
                        term = scaled_ref[r * 3 + c, tile, lanes(block)] * found[c]
                        total = term if total is None else total + term
                    out_ref[r * 6 + m, first : first + count, lanes(block)] = total[0:count, :]


def regroup_kernel(sums_ref, out_ref):
    total = jnp.sum(sums_ref[...], axis=0, keepdims=True)
    out_ref[...] = jnp.broadcast_to(total, out_ref.shape)


def finish_kernel(sums_ref, raw_ref, table_ref, off_ref, self_ref, rho_ref):
    total = jnp.sum(sums_ref[...], axis=0)
    lane = lax.broadcasted_iota(jnp.int32, (1, LANES), 1)
    latest = jnp.sum(jnp.where(lane < 64, total, 0.0), axis=1, keepdims=True)
    earlier = jnp.sum(jnp.where(lane < 64, 0.0, total), axis=1, keepdims=True)
    rho = jnp.sqrt(latest / (earlier + 1e-05))
    rho_ref[...] = jnp.broadcast_to(rho, rho_ref.shape)
    factor = -(OMEGA / rho)
    for entry in range(raw_ref.shape[0]):
        off_ref[entry] = (factor * raw_ref[entry]).astype(jnp.bfloat16)
    keep = 1.0 - OMEGA / rho
    for row in range(3):
        self_ref[row * 6 : row * 6 + 6, :] = (keep * table_ref[row * 8 : row * 8 + 6, :]).astype(
            jnp.bfloat16
        )


def call(kernel, name, outs, *args, near=None, scratch=()):
    near = len(args) if near is None else near
    return pl.pallas_call(
        kernel,
        name=name,
        out_shape=[
            jax.ShapeDtypeStruct(*out) if len(out) == 2 else pltpu.VMEM(*out[:2]) for out in outs
        ],
        in_specs=[VM] * near + [HB] * (len(args) - near),
        out_specs=[VM] * len(outs),
        scratch_shapes=list(scratch),
        compiler_params=pltpu.CompilerParams(vmem_limit_bytes=16 << 20),
    )(*args)


def far(array):
    return pltpu.with_memory_space_constraint(array, pltpu.HBM)


def kept(array):
    return pltpu.with_memory_space_constraint(array, pltpu.VMEM)


def swap(count, offset):
    pairs = []
    for i in range(offset, count - 1, 2):
        pairs += [(i, i + 1), (i + 1, i)]
    return pairs


def squares():
    slabs, subs = lax.axis_size("slab"), lax.axis_size(SUB)
    return [
        [(i + p) * subs + j + q for p in (0, 1) for q in (0, 1)]
        for i in range(0, slabs, 2)
        for j in range(0, subs, 2)
    ]


def exchange(a, b, both):
    bo = lax.ppermute(b, "slab", swap(lax.axis_size("slab"), 1))
    ao = lax.ppermute(a, SUB, swap(lax.axis_size(SUB), 1))
    return ao, bo, lax.all_gather(both, SLAB_SUB, axis_index_groups=squares())


def body(near_null, aggregates, diag_block, off_blocks, columns, sends, start_vector):
    nodes = near_null.shape[1]
    slots = off_blocks.shape[0]
    padded = (slots + 7) // 8 * 8
    subs, slabs = lax.axis_size(SUB), lax.axis_size("slab")
    kept_f32 = lambda *shape: (shape, F32, "kept")
    kept_i32 = lambda *shape: (shape, jnp.int32, "kept")
    table, w, send, a, b, both, scaled, index, side = call(
        start_kernel,
        "start",
        [kept_f32(24, nodes), kept_f32(8, nodes), kept_i32(2, LANES)]
        + [kept_f32(24, LANES)] * 2
        + [kept_f32(48, LANES), kept_f32(9, padded, nodes), kept_i32(padded, nodes)]
        + [kept_i32(4, LANES)],
        far(near_null),
        far(aggregates[None, :]),
        far(start_vector),
        far(sends),
        far(diag_block),
        far(jnp.transpose(off_blocks, (1, 0, 2))),
        far(columns),
        near=0,
        scratch=[
            pltpu.VMEM((18, nodes), F32),
            pltpu.VMEM((1, nodes), jnp.int32),
            pltpu.VMEM((3, nodes), F32),
            pltpu.VMEM((4, 64), jnp.int32),
            pltpu.VMEM((9, nodes), F32),
            pltpu.VMEM((9, slots, nodes), F32),
            pltpu.VMEM((slots, nodes), jnp.int32),
        ]
        + [pltpu.SemaphoreType.DMA] * 7,
    )
    received = [kept(x) for x in exchange(a, b, both)]
    side = kept(side)
    first_received = received
    for iteration in range(ITERS):
        last = iteration == ITERS - 1
        outs = [kept_f32(8, nodes)] + [kept_f32(8, LANES)] * 3
        if last:
            outs = [kept_f32(lax.axis_size(FIRST), 1, LANES)]
        result = call(
            functools.partial(step_kernel, iteration == 0, last),
            f"step_{iteration}",
            outs,
            kept(scaled),
            kept(index),
            kept(w),
            side,
            kept(send),
            *received,
        )
        if last:
            (sums,) = result
        else:
            w = result[0]
            received = [kept(x) for x in exchange(*result[1:])]
    (raw,) = call(
        blocks_out_kernel,
        "blocks_out",
        [kept_f32(18, slots, nodes)],
        kept(scaled),
        kept(index),
        kept(table),
        side,
        *first_received,
    )
    sums = lax.all_to_all(sums, FIRST, 0, 0, tiled=True)
    (sums,) = call(regroup_kernel, "regroup", [kept_f32(lax.axis_size(SECOND), 1, LANES)], kept(sums))
    sums = lax.all_to_all(sums, SECOND, 0, 0, tiled=True)
    prolong_off, prolong_self, rho = call(
        finish_kernel,
        "finish",
        [((18, slots, nodes), jnp.bfloat16), ((18, nodes), jnp.bfloat16), ((1, LANES), F32)],
        kept(sums),
        kept(raw),
        kept(table),
    )
    return (jnp.transpose(prolong_off, (1, 0, 2)), prolong_self, rho[0, 0])


def solution(mesh):
    torus = Mesh(
        mesh.devices.reshape(mesh.shape["slab"], 8, 4, 2), ("slab", "sub_0", "sub_1", "sub_2")
    )
    placed = (
        P(None, SLAB_SUB),
        P(SLAB_SUB),
        P(None, SLAB_SUB),
        P(None, None, SLAB_SUB),
        P(None, SLAB_SUB),
        P(None, SLAB_SUB),
        P(None, SLAB_SUB),
    )
    return jax.shard_map(
        body,
        mesh=torus,
        in_specs=placed,
        out_specs=(P(None, None, SLAB_SUB), P(None, SLAB_SUB), P()),
        check_vma=False,
    )
```
